8 devices in a mesh: tp: 1 (over z), cp: 8 (over y, x, core).
Axes of the slice: x: 2, y: 2, z: 1, core: 2. Of those that a mesh axis runs over, the one named last changes fastest.
Arguments:
- query: bfloat16 [16, 1536, 28, 128], P(None, 'cp', 'tp')
- keys: bfloat16 [16, 1536, 4, 128], P(None, 'cp', 'tp')
- values: bfloat16 [16, 1536, 4, 128], P(None, 'cp', 'tp')
- positions: int32 [16, 1536], P(None, 'cp')
- grad_out: bfloat16 [16, 1536, 28, 128], P(None, 'cp', 'tp')
Outputs:
- output 1: bfloat16 [16, 1536, 28, 128], P(None, 'cp', 'tp')
- output 2: bfloat16 [16, 1536, 28, 128], P(None, 'cp', 'tp')
- output 3: bfloat16 [16, 1536, 4, 128], P(None, 'cp', 'tp')
- output 4: bfloat16 [16, 1536, 4, 128], P(None, 'cp', 'tp')
All inputs are finite; a program needn't handle non-finite values.
Results may differ from the reference program's by a relative error of at most 0.00825609.
Values are sent between devices in bfloat16 or wider.
A program may use at most 1 GiB of HBM per device.

```python
import jax
import jax.numpy as jnp
from jax import lax

BATCH = 16
SEQ_LEN = 1536
CP_SIZE = 8
PART_HEADS = 28
PART_KV_HEADS = 4
HEAD_DIM = 128
ROPE_THETA = 1000000
QUERY_BLOCK = 128

GROUP_SIZE = PART_HEADS // PART_KV_HEADS
LOCAL_LEN = SEQ_LEN // CP_SIZE
HALF_LEN = LOCAL_LEN // 2
NUM_BLOCKS = SEQ_LEN // QUERY_BLOCK


def layout_index():
    stored = jnp.arange(SEQ_LEN, dtype=jnp.int32)
    device = stored // LOCAL_LEN
    within = stored % LOCAL_LEN
    piece_id = jnp.where(within < HALF_LEN, device, 2 * CP_SIZE - 1 - device)
    return piece_id * HALF_LEN + within % HALF_LEN


def draw_positions(pos_key):
    offset_key, gap_key = jax.random.split(pos_key)
    offsets = jax.random.randint(offset_key, (BATCH, 1), 0, SEQ_LEN, dtype=jnp.int32)
    gaps = jax.random.randint(gap_key, (BATCH, SEQ_LEN), 1, 3, dtype=jnp.int32)
    seq_pos = offsets + jnp.cumsum(gaps, axis=1) - gaps[:, :1]
    return jnp.take(seq_pos, layout_index(), axis=1)


def setup_inputs(seed: int = 0, part: int = 0) -> dict:
    base_key = jax.random.key(seed)
    shared_key, part_root = jax.random.split(base_key)
    part_key = jax.random.fold_in(part_root, part)
    key_query, key_keys, key_values, key_grad = jax.random.split(part_key, 4)
    q_shape = (BATCH, SEQ_LEN, PART_HEADS, HEAD_DIM)
    kv_shape = (BATCH, SEQ_LEN, PART_KV_HEADS, HEAD_DIM)
    return {
        'query': jax.random.normal(key_query, q_shape, jnp.float32).astype(jnp.bfloat16),
        'keys': jax.random.normal(key_keys, kv_shape, jnp.float32).astype(jnp.bfloat16),
        'values': jax.random.normal(key_values, kv_shape, jnp.float32).astype(jnp.bfloat16),
        'positions': draw_positions(shared_key),
        'grad_out': jax.random.normal(key_grad, q_shape, jnp.float32).astype(jnp.bfloat16),
    }


def rotary(tensor, positions, angle_sign):
    half_dim = HEAD_DIM // 2
    freq_expo = jnp.arange(half_dim, dtype=jnp.float32) * (2.0 / HEAD_DIM)
    inv_freq = 1.0 / (ROPE_THETA ** freq_expo)
    angles = positions.astype(jnp.float32)[:, :, None] * inv_freq
    cosine = jnp.cos(angles)[:, :, None, :]
    sine_val = angle_sign * jnp.sin(angles)[:, :, None, :]
    pairs = tensor.astype(jnp.float32).reshape(tensor.shape[:-1] + (half_dim, 2))
    even_part = pairs[..., 0]
    odd_part = pairs[..., 1]
    new_even = even_part * cosine - odd_part * sine_val
    new_odd = even_part * sine_val + odd_part * cosine
    return jnp.stack([new_even, new_odd], axis=-1).reshape(tensor.shape)


def reference(query, keys, values, positions, grad_out):
    score_scale = HEAD_DIM ** -0.5
    q_rot = rotary(query, positions, 1.0).astype(jnp.bfloat16)
    k_rot = rotary(keys, positions, 1.0).astype(jnp.bfloat16)

    def by_group(tensor):
        grouped = tensor.reshape(BATCH, NUM_BLOCKS, QUERY_BLOCK, PART_KV_HEADS, GROUP_SIZE, HEAD_DIM)
        grouped = grouped.transpose(0, 3, 1, 2, 4, 5)
        return grouped.reshape(BATCH * PART_KV_HEADS, NUM_BLOCKS, QUERY_BLOCK, GROUP_SIZE, HEAD_DIM)

    def by_kv(tensor):
        return tensor.transpose(0, 2, 1, 3).reshape(BATCH * PART_KV_HEADS, SEQ_LEN, HEAD_DIM)

    pos_rows = jnp.repeat(positions, PART_KV_HEADS, axis=0)

    def one_group(operands):
        q_blocks, k_group, v_group, g_blocks, pos_group = operands
        k_wide = k_group.astype(jnp.float32)
        v_wide = v_group.astype(jnp.float32)
        qpos_blocks = pos_group.reshape(NUM_BLOCKS, QUERY_BLOCK)

        def block_step(acc_pair, blk_inputs):
            dk_acc, dv_acc = acc_pair
            q_blk, g_blk, q_pos = blk_inputs
            q_wide = q_blk.astype(jnp.float32)
            g_wide = g_blk.astype(jnp.float32)
            scores = jnp.einsum('qgd,kd->gqk', q_wide, k_wide) * score_scale
            visible = pos_group[None, :] <= q_pos[:, None]
            scores = jnp.where(visible[None], scores, -jnp.inf)
            weights = jax.nn.softmax(scores, axis=-1)
            out_blk = jnp.einsum('gqk,kd->qgd', weights, v_wide)
            grad_weights = jnp.einsum('qgd,kd->gqk', g_wide, v_wide)
            row_delta = jnp.sum(weights * grad_weights, axis=-1, keepdims=True)
            grad_scores = weights * (grad_weights - row_delta) * score_scale
            dq_blk = jnp.einsum('gqk,kd->qgd', grad_scores, k_wide)
            dk_acc = dk_acc + jnp.einsum('gqk,qgd->kd', grad_scores, q_wide)
            dv_acc = dv_acc + jnp.einsum('gqk,qgd->kd', weights, g_wide)
            return (dk_acc, dv_acc), (out_blk, dq_blk)

        zero_kv = jnp.zeros((SEQ_LEN, HEAD_DIM), jnp.float32)
        sums, per_block = lax.scan(block_step, (zero_kv, zero_kv), (q_blocks, g_blocks, qpos_blocks))
        return per_block[0], per_block[1], sums[0], sums[1]

    out_all, dq_all, dk_all, dv_all = lax.map(
        one_group, (by_group(q_rot), by_kv(k_rot), by_kv(values), by_group(grad_out), pos_rows))

    def from_group(tensor):
        grouped = tensor.reshape(BATCH, PART_KV_HEADS, NUM_BLOCKS, QUERY_BLOCK, GROUP_SIZE, HEAD_DIM)
        return grouped.transpose(0, 2, 3, 1, 4, 5).reshape(BATCH, SEQ_LEN, PART_HEADS, HEAD_DIM)

    def from_kv(tensor):
        return tensor.reshape(BATCH, PART_KV_HEADS, SEQ_LEN, HEAD_DIM).transpose(0, 2, 1, 3)

    attn_out = from_group(out_all).astype(jnp.bfloat16)
    grad_query = rotary(from_group(dq_all), positions, -1.0).astype(jnp.bfloat16)
    grad_keys = rotary(from_kv(dk_all), positions, -1.0).astype(jnp.bfloat16)
    grad_values = from_kv(dv_all).astype(jnp.bfloat16)
    return (attn_out, grad_query, grad_keys, grad_values)
```

```python
import functools

import jax
import jax.numpy as jnp
from jax import lax
from jax.experimental import pallas as pl
from jax.experimental.pallas import tpu as pltpu
from jax.sharding import PartitionSpec as P

ROPE_THETA = 1000000.0
LOG2E = 1.4426950408889634
F32, BF16 = jnp.float32, jnp.bfloat16
KEY_BLOCK = 256
CHUNKS = 4


def swap_pairs(x):
    axis = x.ndim - 1
    lane = lax.broadcasted_iota(jnp.int32, x.shape, axis)
    return jnp.where(lane % 2 == 0, pltpu.roll(x, x.shape[-1] - 1, axis), pltpu.roll(x, 1, axis))


def attend_kernel(info, q_own, q_far, g_own, g_far, cos_own, sin_own, cos_far, sin_far,
                  kv_own, kv_x, kv_y, k_d, v_d, *rest, aliased):
    if aliased:
        rest = rest[2:]
    (o_own, dq_own, o_far, dq_far, dk_own, dv_own, dk_x, dv_x, dk_y, dv_y, dk_d, dv_d,
     qs, gs, kf, vf, dkf, dvf, s_sc, p_sc, acc, dq_acc, inv_sc, row_sc) = rest
    core = info[0]
    chip = info[1]
    _, group, length, dim = q_own.shape
    half = length // 2
    rows = group * length
    seq = kf.shape[0]
    n_low = seq // length - 1
    scale = dim ** -0.5

    for part in range(2):
        src = pl.ds(part * half, half)
        for side, q_ref, g_ref, cos_ref, sin_ref in ((0, q_own, g_own, cos_own, sin_own), (1, q_far, g_far, cos_far, sin_far)):
            dst = pl.ds(side * half, half)
            x = q_ref[0, :, src, :].astype(F32)
            qs[part, :, dst, :] = (x * cos_ref[0, src, :][None] + swap_pairs(x) * sin_ref[0, src, :][None]).astype(BF16)
            gs[part, :, dst, :] = g_ref[0, :, src, :]

    parts = ((1, kv_own.at[0], kv_own.at[1], dk_own, dv_own), (2, kv_x.at[0], kv_x.at[1], dk_x, dv_x),
             (3, kv_y.at[0], kv_y.at[1], dk_y, dv_y), (4, k_d, v_d, dk_d, dv_d))
    for at, k_ref, v_ref, _, _ in parts:
        for which in range(2):
            start = info[at] * length if which == 0 else (n_low - info[at]) * length
            to = pl.ds(pl.multiple_of(start, length), length)
            kf[to, :] = k_ref[0, 0, which]
            vf[to, :] = v_ref[0, 0, which]

    for which in (1, 0):
        first = jnp.where(which == 0, chip * length, (n_low - chip) * length)
        n_blocks = (first + length + KEY_BLOCK - 1) // KEY_BLOCK
        n_full = first // KEY_BLOCK
        own_at = first + (core if which == 0 else 1 - core) * half
        far_at = first + (1 - core if which == 0 else core) * half

        def block(j):
            return pl.ds(pl.multiple_of(j * KEY_BLOCK, KEY_BLOCK), KEY_BLOCK)

        def q_rows():
            return qs[which].reshape(rows, dim)

        def g_rows():
            return gs[which].reshape(rows, dim)

        def scores(j, masked):
            s = lax.dot_general(q_rows(), kf[block(j), :], (((1,), (1,)), ((), ())), preferred_element_type=F32)
            if masked:
                key = lax.broadcasted_iota(jnp.int32, (length, KEY_BLOCK), 1) + j * KEY_BLOCK
                row = lax.broadcasted_iota(jnp.int32, (length, KEY_BLOCK), 0)
                row = jnp.where(row < half, row + own_at, row + (far_at - half))
                bias = jnp.where(key <= row, 0.0, -jnp.inf)
                s = (s.reshape(group, length, KEY_BLOCK) + bias[None]).reshape(rows, KEY_BLOCK)
            s_sc[j] = s
            acc[...] = jnp.maximum(acc[...], jnp.maximum(s[:, :128], s[:, 128:]))

        acc[...] = jnp.full_like(acc, -jnp.inf)
        pl.loop(0, n_full)(lambda j: scores(j, False))
        pl.loop(n_full, n_blocks)(lambda j: scores(j, True))
        row_sc[...] = jnp.broadcast_to(jnp.max(acc[...], axis=1, keepdims=True), (rows, dim))
        acc[...] = jnp.zeros_like(acc)
        inv_sc[...] = jnp.zeros_like(inv_sc)

        @pl.loop(0, n_blocks)
        def _weights(j):
            top = row_sc[...]
            s = s_sc[j]
            left = jnp.exp2((s[:, :128] - top) * (scale * LOG2E))
            right = jnp.exp2((s[:, 128:] - top) * (scale * LOG2E))
            inv_sc[...] += left + right
            p = jnp.concatenate([left.astype(BF16), right.astype(BF16)], axis=1)
            p_sc[j] = p
            acc[...] += jnp.dot(p, vf[block(j), :], preferred_element_type=F32)

        inv = jnp.broadcast_to(1.0 / jnp.sum(inv_sc[...], axis=1, keepdims=True), (rows, dim))
        inv_sc[...] = inv
        out = (acc[...] * inv).astype(BF16)
        delta = jnp.sum(out.astype(F32) * g_rows().astype(F32), axis=1, keepdims=True)
        row_sc[...] = jnp.broadcast_to(delta, (rows, dim))
        dst = pl.ds(which * half, half)
        out = out.reshape(group, length, dim)
        o_own[0, :, dst, :] = out[:, :half]
        o_far[0, :, dst, :] = out[:, half:]
        dq_acc[...] = jnp.zeros_like(dq_acc)

        @pl.loop(0, n_blocks)
        def _grads(j):
            g = g_rows()
            dp = lax.dot_general(g, vf[block(j), :], (((1,), (1,)), ((), ())), preferred_element_type=F32)
            inv = inv_sc[...]
            delta = row_sc[...]
            p = p_sc[j].astype(F32)
            p_left = p[:, :128] * inv
            p_right = p[:, 128:] * inv
            s_left = p_left * (dp[:, :128] - delta)
            s_right = p_right * (dp[:, 128:] - delta)
            pb = jnp.concatenate([p_left.astype(BF16), p_right.astype(BF16)], axis=1)
            ds = jnp.concatenate([s_left.astype(BF16), s_right.astype(BF16)], axis=1)
            dq_acc[...] += jnp.dot(ds, kf[block(j), :], preferred_element_type=F32)
            dv = lax.dot_general(pb, g, (((0,), (0,)), ((), ())), preferred_element_type=F32)
            dk = lax.dot_general(ds, q_rows(), (((0,), (0,)), ((), ())), preferred_element_type=F32)
            if which == 1:
                dvf[block(j), :] = dv
                dkf[block(j), :] = dk
            else:
                dvf[block(j), :] += dv
                dkf[block(j), :] += dk

        if which == 1:
            @pl.loop(n_blocks, seq // KEY_BLOCK)
            def _clear(j):
                dvf[block(j), :] = jnp.zeros((KEY_BLOCK, dim), F32)
                dkf[block(j), :] = jnp.zeros((KEY_BLOCK, dim), F32)

        dq = (dq_acc[...] * scale).reshape(group, length, dim)
        for side, dq_ref, cos_ref, sin_ref in ((0, dq_own, cos_own, sin_own), (1, dq_far, cos_far, sin_far)):
            x = dq[:, side * half:(side + 1) * half]
            dq_ref[0, :, dst, :] = (x * cos_ref[0, dst, :][None] - swap_pairs(x) * sin_ref[0, dst, :][None]).astype(BF16)

    for at, _, _, dk_ref, dv_ref in parts:
        for which in range(2):
            start = info[at] * length if which == 0 else (n_low - info[at]) * length
            to = pl.ds(pl.multiple_of(start, length), length)
            dk_ref[0, 0, which] = dkf[to, :] * scale
            dv_ref[0, 0, which] = dvf[to, :]


def attend(info, q, g, q_far, g_far, tables, kvs, buffers, n_chunk):
    batch, n_heads, length, dim = q.shape
    n_kv = kvs[0].shape[2]
    group = n_heads // n_kv
    seq = 8 * length
    rows = group * length
    wide = (1, group, length, dim)
    at_base = pl.BlockSpec(wide, lambda b, h, info: (info[5] + b, h, 0, 0))
    local = pl.BlockSpec(wide, lambda b, h, info: (b, h, 0, 0))
    table = pl.BlockSpec((1, length, dim), lambda b, h, info: (b, 0, 0))
    pair = pl.BlockSpec((2, 1, 1, 2, length, dim), lambda b, h, info: (0, b, h, 0, 0, 0))
    single = pl.BlockSpec((1, 1, 2, length, dim), lambda b, h, info: (b, h, 0, 0, 0))
    in_specs = [at_base, local, at_base, local] + [table] * 4 + [pair] * 3 + [single] * 2
    operands = [info, q, q_far, g, g_far, *tables, *kvs]
    aliases = {}
    if buffers is not None:
        in_specs += [pl.BlockSpec(memory_space=pl.ANY)] * 2
        operands += list(buffers)
        aliases = {len(operands) - 2: 0, len(operands) - 1: 1}
    grid_spec = pltpu.PrefetchScalarGridSpec(
        num_scalar_prefetch=1, grid=(n_chunk, n_kv), in_specs=in_specs,
        out_specs=[at_base, at_base, local, local] + [single] * 8,
        scratch_shapes=[pltpu.VMEM((2, group, length, dim), BF16)] * 2
        + [pltpu.VMEM((seq, dim), BF16)] * 2 + [pltpu.VMEM((seq, dim), F32)] * 2
        + [pltpu.VMEM((seq // KEY_BLOCK, rows, KEY_BLOCK), F32), pltpu.VMEM((seq // KEY_BLOCK, rows, KEY_BLOCK), BF16)]
        + [pltpu.VMEM((rows, dim), F32)] * 4)
    full = jax.ShapeDtypeStruct((batch, n_heads, length, dim), BF16)
    some = jax.ShapeDtypeStruct((n_chunk, n_heads, length, dim), BF16)
    part = jax.ShapeDtypeStruct((n_chunk, n_kv, 2, length, dim), F32)
    pairs = n_chunk * n_heads * length * (seq + length)
    return pl.pallas_call(
        functools.partial(attend_kernel, aliased=buffers is not None),
        grid_spec=grid_spec, out_shape=[full, full, some, some] + [part] * 8,
        input_output_aliases=aliases,
        cost_estimate=pl.CostEstimate(flops=12 * pairs * dim, bytes_accessed=n_chunk * 16_000_000, transcendentals=pairs),
        compiler_params=pltpu.CompilerParams(vmem_limit_bytes=56 * 1024 * 1024, dimension_semantics=("arbitrary", "arbitrary")),
        name="attend")(*operands)


def rotary_tables(positions, dim):
    freq = 1.0 / (ROPE_THETA ** (jnp.arange(dim // 2, dtype=F32) * (2.0 / dim)))
    angles = positions.astype(F32)[:, :, None] * freq
    cos, sin = jnp.cos(angles), jnp.sin(angles)
    return jnp.repeat(cos, 2, axis=-1), jnp.stack([-sin, sin], axis=-1).reshape(cos.shape[:-1] + (dim,))


def rotate(x, cos, sin):
    pairs = x.reshape(x.shape[:-1] + (x.shape[-1] // 2, 2))
    return x * cos + pairs[..., ::-1].reshape(x.shape) * sin


def solution(mesh):
    n_dev = mesh.shape['cp']
    head_spec = P(None, 'cp', 'tp', None)
    pos_spec = P(None, 'cp')

    def swap(x, bit):
        return lax.ppermute(x, 'cp', [(i, i ^ bit) for i in range(n_dev)])

    def local_step(query, keys, values, positions, grad_out):
        batch, length, n_heads, dim = query.shape
        half = length // 2
        mine = batch // 2
        n_chunk = mine // CHUNKS
        index = lax.axis_index('cp')
        core, chip = index % 2, index // 2
        my_base, far_base = core * mine, (1 - core) * mine

        cos, sin = rotary_tables(positions, dim)
        q = query.transpose(0, 2, 1, 3)
        g = grad_out.transpose(0, 2, 1, 3)
        kv = jnp.stack([rotate(keys.astype(F32), cos[:, :, None], sin[:, :, None]).astype(BF16), values])
        kv = kv.transpose(0, 1, 3, 2, 4)

        def rows_of(x, start, size, axis=0):
            return lax.dynamic_slice_in_dim(x, start, size, axis)

        kv_mine = rows_of(kv, my_base, mine, 1)
        kv_got = swap(rows_of(kv, far_base, mine, 1), 1)
        tab = jnp.stack([cos, sin])
        tab_mine = rows_of(tab, my_base, mine, 1)
        pos_far = swap(rows_of(positions, far_base, mine), 1)
        tab_far = jnp.stack(rotary_tables(pos_far, dim))

        def in_order(a, b):
            return jnp.where(core == 0, jnp.concatenate([a, b], axis=-2), jnp.concatenate([b, a], axis=-2))
        low = in_order(kv_mine[..., :half, :], kv_got[..., :half, :])
        high = in_order(kv_got[..., half:, :], kv_mine[..., half:, :])
        kv_chip = jnp.stack([low, high], axis=3)

        buffers = None
        far_out, far_dq, totals = [], [], []
        for i in range(CHUNKS):
            at = i * n_chunk
            kv_own = kv_chip[:, at:at + n_chunk]
            kv_x, kv_y = swap(kv_own, 2), swap(kv_own, 4)
            k_d, v_d = swap(kv_y[0], 2), swap(kv_x[1], 4)
            q_far = swap(rows_of(q, far_base + at, n_chunk), 1)
            g_far = swap(rows_of(g, far_base + at, n_chunk), 1)
            tables = (tab_mine[0, at:at + n_chunk], tab_mine[1, at:at + n_chunk],
                      tab_far[0, at:at + n_chunk], tab_far[1, at:at + n_chunk])
            info = jnp.stack([core, chip, chip ^ 1, chip ^ 2, chip ^ 3, my_base + at]).astype(jnp.int32)
            out = attend(info, q, g, q_far, g_far, tables, (kv_own, kv_x, kv_y, k_d, v_d), buffers, n_chunk)
            buffers = out[:2]
            far_out.append(swap(out[2], 1))
            far_dq.append(swap(out[3], 1))
            dk_own, dv_own, dk_x, dv_x, dk_y, dv_y, dk_d, dv_d = out[4:]
            got_k = swap(dk_d, 2)
            got_v = swap(dv_d, 4)
            dk = dk_own + swap(dk_x, 2) + swap(dk_y + got_k, 4)
            dv = dv_own + swap(dv_x + got_v, 2) + swap(dv_y, 4)
            totals.append((dk, dv))
        attn_out, grad_query = buffers
        for i in range(CHUNKS):
            attn_out = lax.dynamic_update_slice_in_dim(attn_out, far_out[i], far_base + i * n_chunk, 0)
            grad_query = lax.dynamic_update_slice_in_dim(grad_query, far_dq[i], far_base + i * n_chunk, 0)

        def split(x):
            x = x.transpose(0, 2, 3, 1, 4)
            low, high = x[:, 0], x[:, 1]
            first, second = (low[:, :half], high[:, half:]), (low[:, half:], high[:, :half])
            own = jnp.where(core == 0, jnp.concatenate(first, 1), jnp.concatenate(second, 1))
            far = jnp.where(core == 0, jnp.concatenate(second, 1), jnp.concatenate(first, 1))
            return own, far

        def finish(x, rotated):
            own, far = split(x)
            if rotated:
                own = rotate(own, tab_mine[0][:, :, None], -tab_mine[1][:, :, None])
                far = rotate(far, tab_far[0][:, :, None], -tab_far[1][:, :, None])
            own, far = own.astype(BF16), swap(far.astype(BF16), 1)
            return jnp.where(core == 0, jnp.concatenate([own, far]), jnp.concatenate([far, own]))

        grad_keys = finish(jnp.concatenate([t[0] for t in totals]), True)
        grad_values = finish(jnp.concatenate([t[1] for t in totals]), False)
        return attn_out.transpose(0, 2, 1, 3), grad_query.transpose(0, 2, 1, 3), grad_keys, grad_values

    return jax.shard_map(local_step, mesh=mesh,
                         in_specs=(head_spec, head_spec, head_spec, pos_spec, head_spec),
                         out_specs=(head_spec, head_spec, head_spec, head_spec), check_vma=False)
```
